256 devices in a mesh: dp: 64 (over x, z, y_hi), ctx: 4 (over y_lo, core).
Axes of the slice: x: 4, y: 4 (y_hi: 2, y_lo: 2; y = y_hi * 2 + y_lo), z: 8, core: 2. Of those that a mesh axis runs over, the one named last changes fastest.
Arguments:
- q_short: bfloat16 [49152, 1024], P('dp', 'ctx'), may hold values from -64 to 64
- k_short: bfloat16 [49152, 1024], P('dp', 'ctx'), may hold values from -8 to 8
- v_short: bfloat16 [49152, 1024], P('dp', 'ctx'), may hold values from -6 to 6
- dout_short: bfloat16 [49152, 1024], P('dp', 'ctx'), may hold values from -6 to 6
- doc_lengths: int32 [64, 8], replicated, may hold values from 1 to 256, as said below
- doc_dest: int32 [64, 8], replicated, may hold values from 0 to 63, as said below
- q_long: bfloat16 [64, 512, 1024], P('dp', 'ctx'), may hold values from -64 to 64
- k_long: bfloat16 [64, 512, 1024], P('dp', 'ctx'), may hold values from -8 to 8
- v_long: bfloat16 [64, 512, 1024], P('dp', 'ctx'), may hold values from -6 to 6
- dout_long: bfloat16 [64, 512, 1024], P('dp', 'ctx'), may hold values from -6 to 6
- block_order: int32 [8], replicated, may hold values from 0 to 7, each once
Outputs:
- out_short: bfloat16 [57344, 1024], P('dp', 'ctx')
- dq_short: bfloat16 [49152, 1024], P('dp', 'ctx')
- dk_short: bfloat16 [49152, 1024], P('dp', 'ctx')
- dv_short: bfloat16 [49152, 1024], P('dp', 'ctx')
- out_long: bfloat16 [64, 512, 1024], P('dp', 'ctx')
- dq_long: bfloat16 [64, 512, 1024], P('dp', 'ctx')
- dk_long: bfloat16 [64, 512, 1024], P('dp', 'ctx')
- dv_long: bfloat16 [64, 512, 1024], P('dp', 'ctx')
The draws below stay inside these ranges and needn't reach their ends.
Inputs may be any that keep to these rules, and one draw needn't show every extreme that they name: `doc_lengths`: row r lists in order the lengths of the documents packed on rank r; each row sums to 768. `doc_dest`: entry [r, j] is r, except that in each pair of ranks r and r + 32 exactly one assigns its last document to the other; such a document has at most 128 tokens, and some has exactly 128. `block_order`: A permutation.
All inputs are finite; a program needn't handle non-finite values.
Results may differ from the reference program's by a relative error of at most 0.015.
Values may be sent and summed in bfloat16 or wider, within the bound.
A program may use at most 64 MiB of HBM per device.

```python
import jax
import jax.numpy as jnp
from jax import lax

HEAD_DIM = 128
HF = 1024
SHORT_DEV = 768
DOCS = 8
CAP = 256
MOVE = 128
LONG_DEV = 128
LONG = 512
N_DP = 64
N_CTX = 4


def joint_draw(key, shape):
    key_q = jax.random.fold_in(key, 101)
    key_k = jax.random.fold_in(key, 102)
    queries = jnp.clip(jax.random.normal(key_q, shape, jnp.float32), -6.0, 6.0)
    keys_out = jnp.clip(jax.random.normal(key_k, shape, jnp.float32), -6.0, 6.0)
    return (queries, keys_out)


def plan_draw(key):
    half = N_DP // 2
    ranks = jnp.arange(N_DP, dtype=jnp.int32)
    flips = jax.random.randint(jax.random.fold_in(key, 201), (half,), 0, 2)
    heavy = jnp.concatenate([flips, 1 - flips]) == 1
    chosen = jax.random.randint(jax.random.fold_in(key, 202), (), 0, half)
    tails = jax.random.randint(jax.random.fold_in(key, 203), (N_DP,), MOVE // 2, MOVE + 1)
    tails = jnp.where(ranks % half == chosen, MOVE, tails)
    big_slot = jax.random.randint(jax.random.fold_in(key, 204), (N_DP,), 0, DOCS - 1)
    shares = jax.random.randint(jax.random.fold_in(key, 205), (N_DP, DOCS), 1, 5)
    slots = jnp.arange(DOCS, dtype=jnp.int32)[None, :]
    low_heavy = SHORT_DEV // 96
    others = (slots != DOCS - 1) & (slots != big_slot[:, None])
    share_sum = jnp.sum(jnp.where(others, shares, 0), axis=1)
    spare = SHORT_DEV - CAP - tails - (DOCS - 2) * low_heavy
    extra = jnp.where(others, spare[:, None] * shares // share_sum[:, None], 0)
    leftover = spare - jnp.sum(extra, axis=1)
    first_other = jnp.where(big_slot == 0, 1, 0)
    extra = extra + jnp.where(slots == first_other[:, None], leftover[:, None], 0)
    heavy_row = jnp.where(others, low_heavy + extra, 0) + jnp.where(slots == big_slot[:, None], CAP, 0) + jnp.where(slots == DOCS - 1, tails[:, None], 0)
    low_light = SHORT_DEV // 24
    spare_light = SHORT_DEV - DOCS * low_light
    light_extra = spare_light * shares // jnp.sum(shares, axis=1, keepdims=True)
    light_left = spare_light - jnp.sum(light_extra, axis=1)
    light_row = low_light + light_extra + jnp.where(slots == 0, light_left[:, None], 0)
    lengths = jnp.where(heavy[:, None], heavy_row, light_row).astype(jnp.int32)
    dest = jnp.where(heavy[:, None] & (slots == DOCS - 1), ((ranks + half) % N_DP)[:, None], ranks[:, None]).astype(jnp.int32)
    return (lengths, dest)


def draw_doc_lengths(key, part):
    return plan_draw(jax.random.fold_in(key, 9))[0]


def draw_doc_dest(key, part):
    return plan_draw(jax.random.fold_in(key, 9))[1]


def draw_q_short(key, part):
    return joint_draw(jax.random.fold_in(key, 5), (N_DP * SHORT_DEV, HF))[0].astype(jnp.bfloat16)


def draw_k_short(key, part):
    return joint_draw(jax.random.fold_in(key, 5), (N_DP * SHORT_DEV, HF))[1].astype(jnp.bfloat16)


def draw_q_long(key, part):
    return joint_draw(jax.random.fold_in(key, 7), (N_DP, LONG, HF))[0].astype(jnp.bfloat16)


def draw_k_long(key, part):
    return joint_draw(jax.random.fold_in(key, 7), (N_DP, LONG, HF))[1].astype(jnp.bfloat16)


def steps_of(own_key, extent, cuts, least, top_value):
    def one(dim, blocks):
        steps = jax.random.uniform(jax.random.fold_in(jax.random.fold_in(own_key, 6), dim), (blocks,), jnp.float32, least / len(cuts), top_value / len(cuts))
        return jnp.repeat(jnp.exp(steps), extent[dim] // blocks).reshape((-1,) + (1,) * (len(extent) - dim - 1))

    loudness = one(*cuts[0])
    for cut in cuts[1:]:
        loudness = loudness * one(*cut)
    return loudness


def normal_values(own_key, shape, width, limit, shards=(), held_as=jnp.bfloat16):
    factor_of = steps_of(own_key, shape, shards, -0.22, 0.18) if shards else 1.0
    result = jax.random.normal(own_key, shape, jnp.float32) * width * factor_of
    return jnp.minimum(jnp.maximum(result, -limit), limit).astype(held_as)


def setup_inputs(seed: int = 0) -> dict:
    streams_of = jax.random.split(jax.random.key(seed), 12)
    return {
        "q_short": draw_q_short(jax.random.fold_in(streams_of[11], 71), 0),
        "k_short": draw_k_short(jax.random.fold_in(streams_of[11], 71), 0),
        "v_short": normal_values(streams_of[2], (N_DP * SHORT_DEV, HF), 1.0, 6.0, ((0, 64), (1, 4))),
        "dout_short": normal_values(streams_of[3], (N_DP * SHORT_DEV, HF), 1.0, 6.0, ((0, 64), (1, 4))),
        "doc_lengths": draw_doc_lengths(jax.random.fold_in(streams_of[11], 71), 0),
        "doc_dest": draw_doc_dest(jax.random.fold_in(streams_of[11], 71), 0),
        "q_long": draw_q_long(jax.random.fold_in(streams_of[11], 71), 0),
        "k_long": draw_k_long(jax.random.fold_in(streams_of[11], 71), 0),
        "v_long": normal_values(streams_of[8], (N_DP, LONG, HF), 1.0, 6.0, ((0, 64), (1, 4))),
        "dout_long": normal_values(streams_of[9], (N_DP, LONG, HF), 1.0, 6.0, ((0, 64), (1, 4))),
        "block_order": jax.random.permutation(streams_of[10], 2 * N_CTX).astype(jnp.int32),
    }


NEG = -1e30


def forward_rows(queries, keys, values, mask, scale):
    scores = jnp.einsum("qhd,khd->hqk", queries.astype(jnp.float32), keys.astype(jnp.float32)) * scale
    scores = jnp.where(mask[None], scores, NEG)
    top = jnp.max(scores, axis=-1, keepdims=True)
    lse = top + jnp.log(jnp.sum(jnp.exp(scores - top), axis=-1, keepdims=True))
    probs = jnp.where(mask[None], jnp.exp(scores - lse), 0.0)
    weights = lax.optimization_barrier(probs.astype(jnp.bfloat16))
    attended = jnp.einsum("hqk,khd->qhd", weights.astype(jnp.float32), values.astype(jnp.float32))
    return attended.astype(jnp.bfloat16), probs, weights


def backward_rows(probs, weights, attended, douts, queries, keys, values, scale):
    dfull = douts.astype(jnp.float32)
    dprobs = jnp.einsum("qhd,khd->hqk", dfull, values.astype(jnp.float32))
    delta = jnp.einsum("qhd,qhd->hq", dfull, attended.astype(jnp.float32))
    grads = probs * (dprobs - delta[:, :, None])
    score_grads = lax.optimization_barrier(grads.astype(jnp.bfloat16)).astype(jnp.float32)
    grad_q = jnp.einsum("hqk,khd->qhd", score_grads, keys.astype(jnp.float32)) * scale
    grad_k = jnp.einsum("hqk,qhd->khd", score_grads, queries.astype(jnp.float32)) * scale
    grad_v = jnp.einsum("hqk,qhd->khd", weights.astype(jnp.float32), dfull)
    return grad_q, grad_k, grad_v


def document_of(length_row, token_count):
    starts = (jnp.cumsum(length_row) - length_row).astype(jnp.int32)
    tokens = jnp.arange(token_count, dtype=jnp.int32)
    return (jnp.sum((tokens[:, None] >= starts[None, :]).astype(jnp.int32), axis=1) - 1).astype(jnp.int32)


def positions(block_order, total, rows):
    half = rows // 2
    index = jnp.arange(total, dtype=jnp.int32)
    onehot = ((index // half)[:, None] == jnp.arange(block_order.shape[0], dtype=jnp.int32)[None, :]).astype(jnp.int32)
    return (jnp.sum(onehot * block_order[None, :], axis=1) * half + index % half).astype(jnp.int32)


def reference(q_short, k_short, v_short, dout_short, doc_lengths, doc_dest, q_long, k_long, v_long, dout_long, block_order):
    scale = HEAD_DIM ** -0.5
    features = q_short.shape[1]
    heads = features // HEAD_DIM
    half = N_DP // 2
    tokens = jnp.arange(SHORT_DEV, dtype=jnp.int32)

    def short_rank(items):
        queries, keys, values, douts, length_row = items
        doc_of = document_of(length_row, SHORT_DEV)
        mask = (doc_of[None, :] == doc_of[:, None]) & (tokens[None, :] <= tokens[:, None])
        shaped = [x.reshape(SHORT_DEV, heads, HEAD_DIM) for x in (queries, keys, values, douts)]
        attended, probs, weights = forward_rows(shaped[0], shaped[1], shaped[2], mask, scale)
        grads = backward_rows(probs, weights, attended, shaped[3], shaped[0], shaped[1], shaped[2], scale)
        outs = [attended] + [g.astype(jnp.bfloat16) for g in grads]
        return tuple(o.reshape(SHORT_DEV, features) for o in outs)

    split = lambda x: x.reshape(N_DP, SHORT_DEV, features)
    attended_all, grad_q, grad_k, grad_v = lax.map(short_rank, (split(q_short), split(k_short), split(v_short), split(dout_short), doc_lengths))
    ranks = jnp.arange(N_DP, dtype=jnp.int32)
    moves = doc_dest[:, DOCS - 1] != ranks
    tails = doc_lengths[:, DOCS - 1].astype(jnp.int32)
    moved = moves[:, None] & (tokens[None, :] >= SHORT_DEV - tails[:, None])
    own = jnp.where(moved[..., None], jnp.zeros((), jnp.bfloat16), attended_all)
    partner = ((ranks + half) % N_DP).astype(jnp.int32)
    incoming = jnp.where(moves[partner], tails[partner], 0).astype(jnp.int32)
    padded = jnp.concatenate([attended_all, jnp.zeros((N_DP, MOVE, features), jnp.bfloat16)], axis=1)
    starts = (SHORT_DEV - tails[partner]).astype(jnp.int32)
    received = jax.vmap(lambda block, start: lax.dynamic_slice_in_dim(block, start, MOVE, 0))(padded[partner], starts)
    slots = jnp.arange(MOVE, dtype=jnp.int32)
    received = jnp.where((slots[None, :] < incoming[:, None])[..., None], received, jnp.zeros((), jnp.bfloat16))
    out_short = jnp.concatenate([own, received], axis=1).reshape(N_DP * (SHORT_DEV + MOVE), features)
    flat = lambda x: x.reshape(N_DP * SHORT_DEV, features)

    place = positions(block_order, LONG, LONG_DEV)
    long_mask = place[None, :] <= place[:, None]

    def long_doc(items):
        queries, keys, values, douts = [x.reshape(LONG, heads, HEAD_DIM) for x in items]
        attended, probs, weights = forward_rows(queries, keys, values, long_mask, scale)
        grads = backward_rows(probs, weights, attended, douts, queries, keys, values, scale)
        outs = [attended] + [g.astype(jnp.bfloat16) for g in grads]
        return tuple(o.reshape(LONG, features) for o in outs)

    out_long, dq_long, dk_long, dv_long = lax.map(long_doc, (q_long, k_long, v_long, dout_long))
    return out_short, flat(grad_q), flat(grad_k), flat(grad_v), out_long, dq_long, dk_long, dv_long
```

```python
import functools
import math

import jax
import jax.numpy as jnp
from jax import lax
from jax.experimental import pallas as pl
from jax.experimental.pallas import tpu as pltpu
from jax.sharding import PartitionSpec as P

D = 128
B = 128
NEG = -1e30
SCALE = D**-0.5
EXP_SCALE = SCALE * math.log2(math.e)
MESH = pl.DeviceIdType.MESH
BF16 = jnp.bfloat16
F32 = jnp.float32


def dot_nt(a, b):
    return lax.dot_general(a, b, (((1,), (1,)), ((), ())), preferred_element_type=F32)


def dot_tn(a, b):
    return lax.dot_general(a, b, (((0,), (0,)), ((), ())), preferred_element_type=F32)


def dot_nn(a, b):
    return lax.dot_general(a, b, (((1,), (0,)), ((), ())), preferred_element_type=F32)


def attend(q, k, v, do, mask):
    scores = mask(dot_nt(q, k))
    top = jnp.max(scores, axis=1, keepdims=True)
    e = jnp.exp2((scores - top) * EXP_SCALE)
    probs = e * (1.0 / jnp.sum(e, axis=1, keepdims=True))
    weights = probs.astype(BF16)
    attended = dot_nn(weights, v).astype(BF16)
    delta = jnp.sum(do.astype(F32) * attended.astype(F32), axis=1, keepdims=True)
    grads = (probs * (dot_nt(do, v) - delta)).astype(BF16)
    grad_q = (dot_nn(grads, k) * SCALE).astype(BF16)
    return attended, grad_q, weights, grads


def kernel(
    ranks,
    qs_hbm, ks_hbm, vs_hbm, ds_hbm, len_ref, dest_ref,
    ql_hbm, kl_hbm, vl_hbm, dl_hbm, order_ref,
    os_ref, dqs_ref, dks_ref, dvs_ref, ol_ref, dql_ref, dkl_ref, dvl_ref,
    short, arrived0, arrived1, placed, result, leaving, w_band, g_band, w_long, g_long, moved,
    short_sem, own_sem, in_send, in_recv, out_send, out_recv, move_send, move_recv,
):
    dp = lax.axis_index("dp")
    me = lax.axis_index("ctx")
    partner = lax.rem(dp + ranks // 2, ranks)
    peers = {2: lax.rem(me + 2, 4), 3: 3 - me, 1: me + 1 - 2 * lax.rem(me, 2)}
    tokens = qs_hbm.shape[0]
    heads = qs_hbm.shape[1] // D
    mine, half = ql_hbm.shape[1], ql_hbm.shape[2]
    rows = mine * half
    arrived = (arrived0, arrived1)
    halves = arrived0.shape[1]
    total = halves * half
    longs = (ql_hbm, kl_hbm, vl_hbm, dl_hbm)
    long_outs = (ol_ref, dql_ref, dkl_ref, dvl_ref)

    short_copies = [
        pltpu.make_async_copy(src, short.at[t], short_sem.at[t])
        for t, src in enumerate((qs_hbm, ks_hbm, vs_hbm, ds_hbm))
    ]
    own_copies = []
    for h in range(heads):
        for t in range(4):
            cols = pl.ds(pl.multiple_of(me * heads * D + h * D, D), D)
            own_copies.append(
                pltpu.make_async_copy(
                    longs[t].at[0, :, :, cols],
                    arrived[h].at[t, pl.ds(me * mine, mine), :, :],
                    own_sem.at[h, t],
                )
            )

    barrier = pltpu.get_barrier_semaphore()
    for peer in peers.values():
        pl.semaphore_signal(barrier, inc=1, device_id=(dp, peer), device_id_type=MESH)
    pl.semaphore_signal(barrier, inc=1, device_id=(partner, me), device_id_type=MESH)
    for copy in short_copies:
        copy.start()
    pl.semaphore_wait(barrier, 4)

    in_copies = {}
    for h in range(heads):
        for r, peer in peers.items():
            for t in range(4):
                cols = pl.ds(pl.multiple_of(peer * heads * D + h * D, D), D)
                copy = pltpu.make_async_remote_copy(
                    src_ref=longs[t].at[0, :, :, cols],
                    dst_ref=arrived[h].at[t, pl.ds(me * mine, mine), :, :],
                    send_sem=in_send.at[h, t, r - 1],
                    recv_sem=in_recv.at[h, t, r - 1],
                    device_id=(dp, peer),
                    device_id_type=MESH,
                )
                copy.start()
                in_copies[h, t, r] = copy
    for copy in own_copies:
        copy.start()
    for copy in short_copies:
        copy.wait()

    row = lax.broadcasted_iota(jnp.int32, (B, B), 0)
    col = lax.broadcasted_iota(jnp.int32, (B, B), 1)
    docs = len_ref.shape[0]
    lengths = [len_ref[j, dp] for j in range(docs)]
    tail = lengths[docs - 1]
    moves = dest_ref[docs - 1, dp] != dp
    tail_moved = jnp.where(moves, tail, 0)
    blocks = tokens // B

    def short_block(n):
        first = max(0, n - 2)
        start = jnp.zeros((B, B), jnp.int32)
        at = 0
        for j in range(docs - 1):
            at = at + lengths[j]
            start = jnp.where(row + n * B >= at, at, start)
        pieces = []
        for b in range(first, n + 1):
            piece = col + b * B >= start
            if b == n:
                piece = piece & (col <= row)
            pieces.append(piece)
        allowed = jnp.concatenate(pieces, axis=1) if len(pieces) > 1 else pieces[0]
        mask = lambda s: jnp.where(allowed, s, NEG)
        here = slice(n * B, (n + 1) * B)
        seen = slice(first * B, (n + 1) * B)
        outs = []
        for h in range(heads):
            c = slice(h * D, (h + 1) * D)
            attended, grad_q, weights, grads = attend(
                short[0, here, c], short[1, seen, c], short[2, seen, c], short[3, here, c], mask
            )
            dqs_ref[here, c] = grad_q
            for b in range(first, n + 1):
                to = slice((n - b) * B, (n - b + 1) * B)
                w_band[h, b, to, :] = weights[:, (b - first) * B : (b - first + 1) * B]
                g_band[h, b, to, :] = grads[:, (b - first) * B : (b - first + 1) * B]
            outs.append(attended)
        return here, jnp.concatenate(outs, axis=1)

    def short_keys(b):
        n = min(3, blocks - b) * B
        here = slice(b * B, (b + 1) * B)
        seen = slice(b * B, b * B + n)
        for h in range(heads):
            c = slice(h * D, (h + 1) * D)
            dks_ref[here, c] = (dot_tn(g_band[h, b, :n, :], short[0, seen, c]) * SCALE).astype(BF16)
            dvs_ref[here, c] = dot_tn(w_band[h, b, :n, :], short[3, seen, c]).astype(BF16)

    here, attended = short_block(blocks - 1)
    pick = (col == row + (B - tail_moved)) & (row < tail_moved)
    moved[...] = dot_nn(pick.astype(F32).astype(BF16), attended).astype(BF16)
    move = pltpu.make_async_remote_copy(
        src_ref=moved,
        dst_ref=os_ref.at[tokens : tokens + B, :],
        send_sem=move_send,
        recv_sem=move_recv,
        device_id=(partner, me),
        device_id_type=MESH,
    )
    move.start()
    keep = jnp.concatenate([row, row], axis=1) < B - tail_moved
    os_ref[here, :] = jnp.where(keep, attended.astype(F32), 0.0).astype(BF16)
    for n in range(blocks - 2, -1, -1):
        here, attended = short_block(n)
        os_ref[here, :] = attended
        short_keys(n + 1)
    short_keys(0)

    order = [order_ref[i] for i in range(halves)]
    found = []
    for p in range(halves):
        at = 0
        for i in range(halves):
            at = jnp.where(order[i] == p, i, at)
        found.append(at)
    lower = col <= row
    out_copies = []

    def store(t, n, value):
        for i in range(B // half):
            result[t, n * (B // half) + i] = value[i * half : (i + 1) * half]

    for h in range(heads):
        for t in range(4):
            own_copies[h * 4 + t].wait()
        for r in peers:
            for t in range(4):
                in_copies[h, t, r].wait_recv()
        for t in range(4):
            for p in range(halves):
                placed[t, p * half : (p + 1) * half, :] = arrived[h][t, found[p]]
        for n in range(total // B):
            here = slice(n * B, (n + 1) * B)
            seen = slice(0, (n + 1) * B)

            def mask(s):
                last = jnp.where(lower, s[:, n * B :], NEG)
                return jnp.concatenate([s[:, : n * B], last], axis=1) if n else last

            attended, grad_q, weights, grads = attend(
                placed[0, here, :], placed[1, seen, :], placed[2, seen, :], placed[3, here, :], mask
            )
            store(0, n, attended)
            store(1, n, grad_q)
            w_long[here, seen] = weights
            g_long[here, seen] = grads
        for b in range(total // B):
            here = slice(b * B, (b + 1) * B)
            rest = slice(b * B, total)
            store(2, b, (dot_tn(g_long[rest, here], placed[0, rest, :]) * SCALE).astype(BF16))
            store(3, b, dot_tn(w_long[rest, here], placed[3, rest, :]).astype(BF16))
        for t in range(4):
            for i in range(halves):
                leaving[h, t, i * half : (i + 1) * half, :] = result[t, order[i]]
        cols = pl.ds(pl.multiple_of(me * heads * D + h * D, D), D)
        for r, peer in peers.items():
            for t in range(4):
                copy = pltpu.make_async_remote_copy(
                    src_ref=leaving.at[h, t, pl.ds(pl.multiple_of(peer * rows, rows), rows), :],
                    dst_ref=long_outs[t].at[0, :, cols],
                    send_sem=out_send.at[h, t, r - 1],
                    recv_sem=out_recv.at[h, t, r - 1],
                    device_id=(dp, peer),
                    device_id_type=MESH,
                )
                copy.start()
                out_copies.append(copy)
        for t in range(4):
            long_outs[t][0, :, cols] = leaving[h, t, pl.ds(pl.multiple_of(me * rows, rows), rows), :]

    for copy in in_copies.values():
        copy.wait_send()
    move.wait()
    for copy in out_copies:
        copy.wait()


def settle(*refs):
    count = (len(refs) - 1) // 2
    copies = [
        pltpu.make_async_copy(refs[i], refs[count + i], refs[-1].at[i]) for i in range(count)
    ]
    for copy in copies:
        copy.start()
    for copy in copies:
        copy.wait()


def shards(*args):
    q_short, q_long = args[0], args[6]
    halves = args[10].shape[0]
    tokens, width = q_short.shape
    heads = width // D
    _, rows, wide = q_long.shape
    ctx = lax.axis_size("ctx")
    total = rows * ctx
    blocks = tokens // B
    cut = [a.reshape(1, halves // ctx, total // halves, wide) for a in args[6:10]]
    args = args[:4] + (args[4].T, args[5].T, *cut, args[10])
    vmem = pl.BlockSpec(memory_space=pltpu.VMEM)
    smem = pl.BlockSpec(memory_space=pltpu.SMEM)
    hbm = pl.BlockSpec(memory_space=pl.ANY)
    dma = pltpu.SemaphoreType.DMA
    shapes = [(tokens + B, width)] + [(tokens, width)] * 3 + [(1, rows, wide)] * 4
    outs = pl.pallas_call(
        functools.partial(kernel, lax.axis_size("dp")),
        out_shape=tuple(pltpu.VMEM(s, BF16) for s in shapes),
        in_specs=[hbm] * 4 + [smem] * 2 + [hbm] * 4 + [smem],
        out_specs=(vmem,) * 8,
        scratch_shapes=[
            pltpu.VMEM((4, tokens, width), BF16),
            pltpu.VMEM((4, halves, total // halves, D), BF16),
            pltpu.VMEM((4, halves, total // halves, D), BF16),
            pltpu.VMEM((4, total, D), BF16),
            pltpu.VMEM((4, halves, total // halves, D), BF16),
            pltpu.VMEM((heads, 4, total, D), BF16),
            pltpu.VMEM((heads, blocks, 3 * B, B), BF16),
            pltpu.VMEM((heads, blocks, 3 * B, B), BF16),
            pltpu.VMEM((total, total), BF16),
            pltpu.VMEM((total, total), BF16),
            pltpu.VMEM((B, width), BF16),
            dma((4,)),
            dma((heads, 4)),
            dma((heads, 4, 3)),
            dma((heads, 4, 3)),
            dma((heads, 4, 3)),
            dma((heads, 4, 3)),
            dma,
            dma,
        ],
        compiler_params=pltpu.CompilerParams(collective_id=0, has_side_effects=True),
        name="attention",
    )(*args)
    return pl.pallas_call(
        settle,
        out_shape=tuple(jax.ShapeDtypeStruct(s, BF16) for s in shapes),
        in_specs=[vmem] * 8,
        out_specs=(hbm,) * 8,
        scratch_shapes=[dma((8,))],
        name="settle",
    )(*[pltpu.with_memory_space_constraint(o, pltpu.VMEM) for o in outs])


def solution(mesh):
    short = P("dp", "ctx")
    long = P("dp", "ctx", None)
    return jax.shard_map(
        shards,
        mesh=mesh,
        in_specs=(short,) * 4 + (P(), P()) + (long,) * 4 + (P(),),
        out_specs=(short,) * 4 + (long,) * 4,
        check_vma=False,
    )
```

```python
import functools
import math

import jax
import jax.numpy as jnp
from jax import lax
from jax.experimental import pallas as pl
from jax.experimental.pallas import tpu as pltpu
from jax.sharding import PartitionSpec as P

D = 128
B = 128
NEG = -1e30
SCALE = D**-0.5
EXP_SCALE = SCALE * math.log2(math.e)
MESH = pl.DeviceIdType.MESH
BF16 = jnp.bfloat16
F32 = jnp.float32


def dot_nt(a, b):
    return lax.dot_general(a, b, (((1,), (1,)), ((), ())), preferred_element_type=F32)


def dot_tn(a, b):
    return lax.dot_general(a, b, (((0,), (0,)), ((), ())), preferred_element_type=F32)


def dot_nn(a, b):
    return lax.dot_general(a, b, (((1,), (0,)), ((), ())), preferred_element_type=F32)


def attend(q, k, v, do, mask):
    scores = mask(dot_nt(q, k))
    top = jnp.max(scores, axis=1, keepdims=True)
    e = jnp.exp2((scores - top) * EXP_SCALE)
    probs = e * (1.0 / jnp.sum(e, axis=1, keepdims=True))
    weights = probs.astype(BF16)
    attended = dot_nn(weights, v).astype(BF16)
    delta = jnp.sum(do.astype(F32) * attended.astype(F32), axis=1, keepdims=True)
    grads = (probs * (dot_nt(do, v) - delta)).astype(BF16)
    grad_q = (dot_nn(grads, k) * SCALE).astype(BF16)
    return attended, grad_q, weights, grads


def kernel(
    ranks,
    qs_hbm, ks_hbm, vs_hbm, ds_hbm, len_hbm, dest_hbm,
    ql_hbm, kl_hbm, vl_hbm, dl_hbm, order_hbm,
    os_ref, dqs_ref, dks_ref, dvs_ref, ol_ref, dql_ref, dkl_ref, dvl_ref,
    len_ref, dest_ref, order_ref, staged, short, arrived0, arrived1, placed, result, leaving, w_band, g_band, w_long, g_long, moved,
    int_sem, stage_sem, short_sem, own_sem, in_send, in_recv, out_send, out_recv, move_send, move_recv,
):
    dp = lax.axis_index("dp")
    me = lax.axis_index("ctx")
    partner = lax.rem(dp + ranks // 2, ranks)
    peers = {2: lax.rem(me + 2, 4), 3: 3 - me, 1: me + 1 - 2 * lax.rem(me, 2)}
    tokens = qs_hbm.shape[0]
    heads = qs_hbm.shape[1] // D
    mine, half = ql_hbm.shape[1], ql_hbm.shape[2]
    rows = mine * half
    arrived = (arrived0, arrived1)
    halves = arrived0.shape[1]
    total = halves * half
    longs = (ql_hbm, kl_hbm, vl_hbm, dl_hbm)
    long_outs = (ol_ref, dql_ref, dkl_ref, dvl_ref)

    int_copies = [
        pltpu.make_async_copy(src, dst, int_sem.at[i])
        for i, (src, dst) in enumerate(
            ((len_hbm, len_ref), (dest_hbm, dest_ref), (order_hbm, order_ref))
        )
    ]
    stage_copies = [
        pltpu.make_async_copy(longs[t], staged.at[t], stage_sem.at[t]) for t in range(4)
    ]
    short_copies = [
        pltpu.make_async_copy(src, short.at[t], short_sem.at[t])
        for t, src in enumerate((qs_hbm, ks_hbm, vs_hbm, ds_hbm))
    ]
    own_copies = []
    for h in range(heads):
        for t in range(4):
            cols = pl.ds(pl.multiple_of(me * heads * D + h * D, D), D)
            own_copies.append(
                pltpu.make_async_copy(
                    longs[t].at[0, :, :, cols],
                    arrived[h].at[t, pl.ds(me * mine, mine), :, :],
                    own_sem.at[h, t],
                )
            )

    barrier = pltpu.get_barrier_semaphore()
    for peer in peers.values():
        pl.semaphore_signal(barrier, inc=1, device_id=(dp, peer), device_id_type=MESH)
    pl.semaphore_signal(barrier, inc=1, device_id=(partner, me), device_id_type=MESH)
    for copy in stage_copies + int_copies + own_copies + short_copies:
        copy.start()
    for copy in stage_copies:
        copy.wait()
    pl.semaphore_wait(barrier, 4)

    in_copies = {}
    for h in range(heads):
        for r, peer in peers.items():
            for t in range(4):
                cols = pl.ds(pl.multiple_of(peer * heads * D + h * D, D), D)
                copy = pltpu.make_async_remote_copy(
                    src_ref=staged.at[t, 0, :, :, cols],
                    dst_ref=arrived[h].at[t, pl.ds(me * mine, mine), :, :],
                    send_sem=in_send.at[h, t, r - 1],
                    recv_sem=in_recv.at[h, t, r - 1],
                    device_id=(dp, peer),
                    device_id_type=MESH,
                )
                copy.start()
                in_copies[h, t, r] = copy
    for copy in int_copies + short_copies:
        copy.wait()

    row = lax.broadcasted_iota(jnp.int32, (B, B), 0)
    col = lax.broadcasted_iota(jnp.int32, (B, B), 1)
    docs = len_ref.shape[0]
    lengths = [len_ref[j, dp] for j in range(docs)]
    tail = lengths[docs - 1]
    moves = dest_ref[docs - 1, dp] != dp
    tail_moved = jnp.where(moves, tail, 0)
    blocks = tokens // B

    def short_block(n):
        first = max(0, n - 2)
        start = jnp.zeros((B, B), jnp.int32)
        at = 0
        for j in range(docs - 1):
            at = at + lengths[j]
            start = jnp.where(row + n * B >= at, at, start)
        pieces = []
        for b in range(first, n + 1):
            piece = col + b * B >= start
            if b == n:
                piece = piece & (col <= row)
            pieces.append(piece)
        allowed = jnp.concatenate(pieces, axis=1) if len(pieces) > 1 else pieces[0]
        mask = lambda s: jnp.where(allowed, s, NEG)
        here = slice(n * B, (n + 1) * B)
        seen = slice(first * B, (n + 1) * B)
        outs = []
        for h in range(heads):
            c = slice(h * D, (h + 1) * D)
            attended, grad_q, weights, grads = attend(
                short[0, here, c], short[1, seen, c], short[2, seen, c], short[3, here, c], mask
            )
            dqs_ref[here, c] = grad_q
            for b in range(first, n + 1):
                to = slice((n - b) * B, (n - b + 1) * B)
                w_band[h, b, to, :] = weights[:, (b - first) * B : (b - first + 1) * B]
                g_band[h, b, to, :] = grads[:, (b - first) * B : (b - first + 1) * B]
            outs.append(attended)
        return here, jnp.concatenate(outs, axis=1)

    def short_keys(b):
        n = min(3, blocks - b) * B
        here = slice(b * B, (b + 1) * B)
        seen = slice(b * B, b * B + n)
        for h in range(heads):
            c = slice(h * D, (h + 1) * D)
            dks_ref[here, c] = (dot_tn(g_band[h, b, :n, :], short[0, seen, c]) * SCALE).astype(BF16)
            dvs_ref[here, c] = dot_tn(w_band[h, b, :n, :], short[3, seen, c]).astype(BF16)

    here, attended = short_block(blocks - 1)
    pick = (col == row + (B - tail_moved)) & (row < tail_moved)
    moved[...] = dot_nn(pick.astype(F32).astype(BF16), attended).astype(BF16)
    move = pltpu.make_async_remote_copy(
        src_ref=moved,
        dst_ref=os_ref.at[tokens : tokens + B, :],
        send_sem=move_send,
        recv_sem=move_recv,
        device_id=(partner, me),
        device_id_type=MESH,
    )
    move.start()
    keep = jnp.concatenate([row, row], axis=1) < B - tail_moved
    os_ref[here, :] = jnp.where(keep, attended.astype(F32), 0.0).astype(BF16)
    for n in range(blocks - 2, -1, -1):
        here, attended = short_block(n)
        os_ref[here, :] = attended
        short_keys(n + 1)
    short_keys(0)

    order = [order_ref[i] for i in range(halves)]
    found = []
    for p in range(halves):
        at = 0
        for i in range(halves):
            at = jnp.where(order[i] == p, i, at)
        found.append(at)
    lower = col <= row
    out_copies = {}

    def store(t, n, value):
        for i in range(B // half):
            result[t, n * (B // half) + i] = value[i * half : (i + 1) * half]

    for h in range(heads):
        for t in range(4):
            own_copies[h * 4 + t].wait()
        for r in peers:
            for t in range(4):
                in_copies[h, t, r].wait_recv()
        for t in range(4):
            for p in range(halves):
                placed[t, p * half : (p + 1) * half, :] = arrived[h][t, found[p]]
        for n in range(total // B):
            here = slice(n * B, (n + 1) * B)
            seen = slice(0, (n + 1) * B)

            def mask(s):
                last = jnp.where(lower, s[:, n * B :], NEG)
                return jnp.concatenate([s[:, : n * B], last], axis=1) if n else last

            attended, grad_q, weights, grads = attend(
                placed[0, here, :], placed[1, seen, :], placed[2, seen, :], placed[3, here, :], mask
            )
            store(0, n, attended)
            store(1, n, grad_q)
            w_long[here, seen] = weights
            g_long[here, seen] = grads
        for b in range(total // B):
            here = slice(b * B, (b + 1) * B)
            rest = slice(b * B, total)
            store(2, b, (dot_tn(g_long[rest, here], placed[0, rest, :]) * SCALE).astype(BF16))
            store(3, b, dot_tn(w_long[rest, here], placed[3, rest, :]).astype(BF16))
        for t in range(4):
            for i in range(halves):
                leaving[h, t, i * half : (i + 1) * half, :] = result[t, order[i]]
        cols = pl.ds(pl.multiple_of(me * heads * D + h * D, D), D)
        for r, peer in peers.items():
            for t in range(4):
                copy = pltpu.make_async_remote_copy(
                    src_ref=leaving.at[h, t, pl.ds(pl.multiple_of(peer * rows, rows), rows), :],
                    dst_ref=long_outs[t].at[0, :, cols],
                    send_sem=out_send.at[h, t, r - 1],
                    recv_sem=out_recv.at[h, t, r - 1],
                    device_id=(dp, peer),
                    device_id_type=MESH,
                )
                copy.start()
                out_copies[h, t, r] = copy
        for t in range(4):
            long_outs[t][0, :, cols] = leaving[h, t, pl.ds(pl.multiple_of(me * rows, rows), rows), :]

    for copy in in_copies.values():
        copy.wait_send()
    move.wait()
    for r in (1, 2, 3):
        for h in range(heads):
            for t in range(4):
                out_copies[h, t, r].wait_send()
    for r in (1, 2, 3):
        for h in range(heads):
            for t in range(4):
                out_copies[h, t, r].wait_recv()


def settle(*refs):
    count = (len(refs) - 1) // 2
    copies = [
        pltpu.make_async_copy(refs[i], refs[count + i], refs[-1].at[i]) for i in range(count)
    ]
    for copy in copies:
        copy.start()
    for copy in copies:
        copy.wait()


def shards(*args):
    q_short, q_long = args[0], args[6]
    halves = args[10].shape[0]
    tokens, width = q_short.shape
    heads = width // D
    _, rows, wide = q_long.shape
    ctx = lax.axis_size("ctx")
    total = rows * ctx
    blocks = tokens // B
    cut = [a.reshape(1, halves // ctx, total // halves, wide) for a in args[6:10]]
    args = args[:4] + (args[4].T, args[5].T, *cut, args[10])
    vmem = pl.BlockSpec(memory_space=pltpu.VMEM)
    hbm = pl.BlockSpec(memory_space=pl.ANY)
    dma = pltpu.SemaphoreType.DMA
    shapes = [(tokens + B, width)] + [(tokens, width)] * 3 + [(1, rows, wide)] * 4
    outs = pl.pallas_call(
        functools.partial(kernel, lax.axis_size("dp")),
        out_shape=tuple(pltpu.VMEM(s, BF16) for s in shapes),
        in_specs=[hbm] * 11,
        out_specs=(vmem,) * 8,
        scratch_shapes=[
            pltpu.SMEM(args[4].shape, jnp.int32),
            pltpu.SMEM(args[5].shape, jnp.int32),
            pltpu.SMEM(args[10].shape, jnp.int32),
            pltpu.VMEM((4,) + cut[0].shape, BF16),
            pltpu.VMEM((4, tokens, width), BF16),
            pltpu.VMEM((4, halves, total // halves, D), BF16),
            pltpu.VMEM((4, halves, total // halves, D), BF16),
            pltpu.VMEM((4, total, D), BF16),
            pltpu.VMEM((4, halves, total // halves, D), BF16),
            pltpu.VMEM((heads, 4, total, D), BF16),
            pltpu.VMEM((heads, blocks, 3 * B, B), BF16),
            pltpu.VMEM((heads, blocks, 3 * B, B), BF16),
            pltpu.VMEM((total, total), BF16),
            pltpu.VMEM((total, total), BF16),
            pltpu.VMEM((B, width), BF16),
            dma((3,)),
            dma((4,)),
            dma((4,)),
            dma((heads, 4)),
            dma((heads, 4, 3)),
            dma((heads, 4, 3)),
            dma((heads, 4, 3)),
            dma((heads, 4, 3)),
            dma,
            dma,
        ],
        compiler_params=pltpu.CompilerParams(collective_id=0, has_side_effects=True),
        name="attention",
    )(*args)
    return pl.pallas_call(
        settle,
        out_shape=tuple(jax.ShapeDtypeStruct(s, BF16) for s in shapes),
        in_specs=[vmem] * 8,
        out_specs=(hbm,) * 8,
        scratch_shapes=[dma((8,))],
        name="settle",
    )(*[pltpu.with_memory_space_constraint(o, pltpu.VMEM) for o in outs])


def solution(mesh):
    short = P("dp", "ctx")
    long = P("dp", "ctx", None)
    return jax.shard_map(
        shards,
        mesh=mesh,
        in_specs=(short,) * 4 + (P(), P()) + (long,) * 4 + (P(),),
        out_specs=(short,) * 4 + (long,) * 4,
        check_vma=False,
    )
```

```python
import functools
import math

import jax
import jax.numpy as jnp
from jax import lax
from jax.experimental import pallas as pl
from jax.experimental.pallas import tpu as pltpu
from jax.sharding import PartitionSpec as P

D = 128
B = 128
NEG = -1e30
LEADER = 1
SCALE = D**-0.5
EXP_SCALE = SCALE * math.log2(math.e)
MESH = pl.DeviceIdType.MESH
BF16 = jnp.bfloat16
F32 = jnp.float32


def dot_nt(a, b):
    return lax.dot_general(a, b, (((1,), (1,)), ((), ())), preferred_element_type=F32)


def dot_tn(a, b):
    return lax.dot_general(a, b, (((0,), (0,)), ((), ())), preferred_element_type=F32)


def dot_nn(a, b):
    return lax.dot_general(a, b, (((1,), (0,)), ((), ())), preferred_element_type=F32)


def attend(q, k, v, do, mask):
    scores = mask(dot_nt(q, k))
    top = jnp.max(scores, axis=1, keepdims=True)
    e = jnp.exp2((scores - top) * EXP_SCALE)
    probs = e * (1.0 / jnp.sum(e, axis=1, keepdims=True))
    weights = probs.astype(BF16)
    attended = dot_nn(weights, v).astype(BF16)
    delta = jnp.sum(do.astype(F32) * attended.astype(F32), axis=1, keepdims=True)
    grads = (probs * (dot_nt(do, v) - delta)).astype(BF16)
    grad_q = (dot_nn(grads, k) * SCALE).astype(BF16)
    return attended, grad_q, weights, grads


def kernel(
    ranks,
    qs_hbm, ks_hbm, vs_hbm, ds_hbm, len_hbm, dest_hbm,
    ql_hbm, kl_hbm, vl_hbm, dl_hbm, order_hbm,
    os_ref, dqs_ref, dks_ref, dvs_ref, ol_ref, dql_ref, dkl_ref, dvl_ref,
    len_ref, dest_ref, order_ref, staged, short, arrived0, arrived1, placed, result, leaving, w_band, g_band, w_long, g_long, moved,
    int_sem, stage_sem, short_sem, own_sem, in_send, in_recv, out_send, out_recv, move_send, move_recv,
    cross_sem, go_sem,
):
    dp = lax.axis_index("dp")
    me = lax.axis_index("ctx")
    partner = lax.rem(dp + ranks // 2, ranks)
    peers = {2: lax.rem(me + 2, 4), 3: 3 - me, 1: me + 1 - 2 * lax.rem(me, 2)}
    tokens = qs_hbm.shape[0]
    heads = qs_hbm.shape[1] // D
    mine, half = ql_hbm.shape[1], ql_hbm.shape[2]
    rows = mine * half
    arrived = (arrived0, arrived1)
    halves = arrived0.shape[1]
    total = halves * half
    longs = (ql_hbm, kl_hbm, vl_hbm, dl_hbm)
    long_outs = (ol_ref, dql_ref, dkl_ref, dvl_ref)

    int_copies = [
        pltpu.make_async_copy(src, dst, int_sem.at[i])
        for i, (src, dst) in enumerate(
            ((len_hbm, len_ref), (dest_hbm, dest_ref), (order_hbm, order_ref))
        )
    ]
    stage_copies = [
        pltpu.make_async_copy(longs[t], staged.at[t], stage_sem.at[t]) for t in range(4)
    ]
    short_copies = [
        pltpu.make_async_copy(src, short.at[t], short_sem.at[t])
        for t, src in enumerate((qs_hbm, ks_hbm, vs_hbm, ds_hbm))
    ]
    own_copies = []
    for h in range(heads):
        for t in range(4):
            cols = pl.ds(pl.multiple_of(me * heads * D + h * D, D), D)
            own_copies.append(
                pltpu.make_async_copy(
                    longs[t].at[0, :, :, cols],
                    arrived[h].at[t, pl.ds(me * mine, mine), :, :],
                    own_sem.at[h, t],
                )
            )

    barrier = pltpu.get_barrier_semaphore()
    for peer in peers.values():
        pl.semaphore_signal(barrier, inc=1, device_id=(dp, peer), device_id_type=MESH)

    @pl.when(me == LEADER)
    def _():
        pl.semaphore_signal(barrier, inc=1, device_id=(partner, me), device_id_type=MESH)

    for copy in stage_copies + int_copies + own_copies + short_copies:
        copy.start()
    for copy in stage_copies:
        copy.wait()
    pl.semaphore_wait(barrier, jnp.where(me == LEADER, 4, 3))

    @pl.when(me == LEADER)
    def _():
        pl.semaphore_signal(cross_sem, inc=1, device_id=(partner, me), device_id_type=MESH)


    in_copies = {}
    for h in range(heads):
        for r, peer in peers.items():
            for t in range(4):
                cols = pl.ds(pl.multiple_of(peer * heads * D + h * D, D), D)
                copy = pltpu.make_async_remote_copy(
                    src_ref=staged.at[t, 0, :, :, cols],
                    dst_ref=arrived[h].at[t, pl.ds(me * mine, mine), :, :],
                    send_sem=in_send.at[h, t, r - 1],
                    recv_sem=in_recv.at[h, t, r - 1],
                    device_id=(dp, peer),
                    device_id_type=MESH,
                )
                copy.start()
                in_copies[h, t, r] = copy
    for copy in int_copies + short_copies:
        copy.wait()

    row = lax.broadcasted_iota(jnp.int32, (B, B), 0)
    col = lax.broadcasted_iota(jnp.int32, (B, B), 1)
    docs = len_ref.shape[0]
    lengths = [len_ref[j, dp] for j in range(docs)]
    tail = lengths[docs - 1]
    moves = dest_ref[docs - 1, dp] != dp
    tail_moved = jnp.where(moves, tail, 0)
    blocks = tokens // B

    def short_block(n):
        first = max(0, n - 2)
        start = jnp.zeros((B, B), jnp.int32)
        at = 0
        for j in range(docs - 1):
            at = at + lengths[j]
            start = jnp.where(row + n * B >= at, at, start)
        pieces = []
        for b in range(first, n + 1):
            piece = col + b * B >= start
            if b == n:
                piece = piece & (col <= row)
            pieces.append(piece)
        allowed = jnp.concatenate(pieces, axis=1) if len(pieces) > 1 else pieces[0]
        mask = lambda s: jnp.where(allowed, s, NEG)
        here = slice(n * B, (n + 1) * B)
        seen = slice(first * B, (n + 1) * B)
        outs = []
        for h in range(heads):
            c = slice(h * D, (h + 1) * D)
            attended, grad_q, weights, grads = attend(
                short[0, here, c], short[1, seen, c], short[2, seen, c], short[3, here, c], mask
            )
            dqs_ref[here, c] = grad_q
            for b in range(first, n + 1):
                to = slice((n - b) * B, (n - b + 1) * B)
                w_band[h, b, to, :] = weights[:, (b - first) * B : (b - first + 1) * B]
                g_band[h, b, to, :] = grads[:, (b - first) * B : (b - first + 1) * B]
            outs.append(attended)
        return here, jnp.concatenate(outs, axis=1)

    def short_keys(b):
        n = min(3, blocks - b) * B
        here = slice(b * B, (b + 1) * B)
        seen = slice(b * B, b * B + n)
        for h in range(heads):
            c = slice(h * D, (h + 1) * D)
            dks_ref[here, c] = (dot_tn(g_band[h, b, :n, :], short[0, seen, c]) * SCALE).astype(BF16)
            dvs_ref[here, c] = dot_tn(w_band[h, b, :n, :], short[3, seen, c]).astype(BF16)

    here, attended = short_block(blocks - 1)
    pick = (col == row + (B - tail_moved)) & (row < tail_moved)
    moved[...] = dot_nn(pick.astype(F32).astype(BF16), attended).astype(BF16)
    move = pltpu.make_async_remote_copy(
        src_ref=moved,
        dst_ref=os_ref.at[tokens : tokens + B, :],
        send_sem=move_send,
        recv_sem=move_recv,
        device_id=(partner, me),
        device_id_type=MESH,
    )
    keep = jnp.concatenate([row, row], axis=1) < B - tail_moved
    os_ref[here, :] = jnp.where(keep, attended.astype(F32), 0.0).astype(BF16)
    for n in range(blocks - 2, -1, -1):
        here, attended = short_block(n)
        os_ref[here, :] = attended
        short_keys(n + 1)
        if n == blocks // 2:

            @pl.when(me == LEADER)
            def _():
                pl.semaphore_wait(cross_sem, 1)
                for peer in peers.values():
                    pl.semaphore_signal(go_sem, inc=1, device_id=(dp, peer), device_id_type=MESH)

    short_keys(0)

    @pl.when(me != LEADER)
    def _():
        pl.semaphore_wait(go_sem, 1)

    move.start()

    order = [order_ref[i] for i in range(halves)]
    found = []
    for p in range(halves):
        at = 0
        for i in range(halves):
            at = jnp.where(order[i] == p, i, at)
        found.append(at)
    lower = col <= row
    out_copies = {}

    def store(t, n, value):
        for i in range(B // half):
            result[t, n * (B // half) + i] = value[i * half : (i + 1) * half]

    for h in range(heads):
        for t in range(4):
            own_copies[h * 4 + t].wait()
        for r in peers:
            for t in range(4):
                in_copies[h, t, r].wait_recv()
        for t in range(4):
            for p in range(halves):
                placed[t, p * half : (p + 1) * half, :] = arrived[h][t, found[p]]
        for n in range(total // B):
            here = slice(n * B, (n + 1) * B)
            seen = slice(0, (n + 1) * B)

            def mask(s):
                last = jnp.where(lower, s[:, n * B :], NEG)
                return jnp.concatenate([s[:, : n * B], last], axis=1) if n else last

            attended, grad_q, weights, grads = attend(
                placed[0, here, :], placed[1, seen, :], placed[2, seen, :], placed[3, here, :], mask
            )
            store(0, n, attended)
            store(1, n, grad_q)
            w_long[here, seen] = weights
            g_long[here, seen] = grads
        for b in range(total // B):
            here = slice(b * B, (b + 1) * B)
            rest = slice(b * B, total)
            store(2, b, (dot_tn(g_long[rest, here], placed[0, rest, :]) * SCALE).astype(BF16))
            store(3, b, dot_tn(w_long[rest, here], placed[3, rest, :]).astype(BF16))
        for t in range(4):
            for i in range(halves):
                leaving[h, t, i * half : (i + 1) * half, :] = result[t, order[i]]
        cols = pl.ds(pl.multiple_of(me * heads * D + h * D, D), D)
        for r, peer in peers.items():
            for t in range(4):
                copy = pltpu.make_async_remote_copy(
                    src_ref=leaving.at[h, t, pl.ds(pl.multiple_of(peer * rows, rows), rows), :],
                    dst_ref=long_outs[t].at[0, :, cols],
                    send_sem=out_send.at[h, t, r - 1],
                    recv_sem=out_recv.at[h, t, r - 1],
                    device_id=(dp, peer),
                    device_id_type=MESH,
                )
                copy.start()
                out_copies[h, t, r] = copy
        for t in range(4):
            long_outs[t][0, :, cols] = leaving[h, t, pl.ds(pl.multiple_of(me * rows, rows), rows), :]

    for copy in in_copies.values():
        copy.wait_send()
    move.wait()
    for r in (1, 2, 3):
        for h in range(heads):
            for t in range(4):
                out_copies[h, t, r].wait_send()
    for r in (1, 2, 3):
        for h in range(heads):
            for t in range(4):
                out_copies[h, t, r].wait_recv()


def settle(*refs):
    count = (len(refs) - 1) // 2
    copies = [
        pltpu.make_async_copy(refs[i], refs[count + i], refs[-1].at[i]) for i in range(count)
    ]
    for copy in copies:
        copy.start()
    for copy in copies:
        copy.wait()


def shards(*args):
    q_short, q_long = args[0], args[6]
    halves = args[10].shape[0]
    tokens, width = q_short.shape
    heads = width // D
    _, rows, wide = q_long.shape
    ctx = lax.axis_size("ctx")
    total = rows * ctx
    blocks = tokens // B
    cut = [a.reshape(1, halves // ctx, total // halves, wide) for a in args[6:10]]
    args = args[:4] + (args[4].T, args[5].T, *cut, args[10])
    vmem = pl.BlockSpec(memory_space=pltpu.VMEM)
    hbm = pl.BlockSpec(memory_space=pl.ANY)
    dma = pltpu.SemaphoreType.DMA
    shapes = [(tokens + B, width)] + [(tokens, width)] * 3 + [(1, rows, wide)] * 4
    outs = pl.pallas_call(
        functools.partial(kernel, lax.axis_size("dp")),
        out_shape=tuple(pltpu.VMEM(s, BF16) for s in shapes),
        in_specs=[hbm] * 11,
        out_specs=(vmem,) * 8,
        scratch_shapes=[
            pltpu.SMEM(args[4].shape, jnp.int32),
            pltpu.SMEM(args[5].shape, jnp.int32),
            pltpu.SMEM(args[10].shape, jnp.int32),
            pltpu.VMEM((4,) + cut[0].shape, BF16),
            pltpu.VMEM((4, tokens, width), BF16),
            pltpu.VMEM((4, halves, total // halves, D), BF16),
            pltpu.VMEM((4, halves, total // halves, D), BF16),
            pltpu.VMEM((4, total, D), BF16),
            pltpu.VMEM((4, halves, total // halves, D), BF16),
            pltpu.VMEM((heads, 4, total, D), BF16),
            pltpu.VMEM((heads, blocks, 3 * B, B), BF16),
            pltpu.VMEM((heads, blocks, 3 * B, B), BF16),
            pltpu.VMEM((total, total), BF16),
            pltpu.VMEM((total, total), BF16),
            pltpu.VMEM((B, width), BF16),
            dma((3,)),
            dma((4,)),
            dma((4,)),
            dma((heads, 4)),
            dma((heads, 4, 3)),
            dma((heads, 4, 3)),
            dma((heads, 4, 3)),
            dma((heads, 4, 3)),
            dma,
            dma,
            pltpu.SemaphoreType.REGULAR,
            pltpu.SemaphoreType.REGULAR,
        ],
        compiler_params=pltpu.CompilerParams(collective_id=0, has_side_effects=True),
        name="attention",
    )(*args)
    return pl.pallas_call(
        settle,
        out_shape=tuple(jax.ShapeDtypeStruct(s, BF16) for s in shapes),
        in_specs=[vmem] * 8,
        out_specs=(hbm,) * 8,
        scratch_shapes=[dma((8,))],
        name="settle",
    )(*[pltpu.with_memory_space_constraint(o, pltpu.VMEM) for o in outs])


def solution(mesh):
    short = P("dp", "ctx")
    long = P("dp", "ctx", None)
    return jax.shard_map(
        shards,
        mesh=mesh,
        in_specs=(short,) * 4 + (P(), P()) + (long,) * 4 + (P(),),
        out_specs=(short,) * 4 + (long,) * 4,
        check_vma=False,
    )
```

```python
import functools
import math

import jax
import jax.numpy as jnp
from jax import lax
from jax.experimental import pallas as pl
from jax.experimental.pallas import tpu as pltpu
from jax.sharding import PartitionSpec as P

D = 128
B = 128
NEG = -1e30
LEADER = 2
EARLY = 1
SCALE = D**-0.5
EXP_SCALE = SCALE * math.log2(math.e)
MESH = pl.DeviceIdType.MESH
BF16 = jnp.bfloat16
F32 = jnp.float32


def dot_nt(a, b):
    return lax.dot_general(a, b, (((1,), (1,)), ((), ())), preferred_element_type=F32)


def dot_tn(a, b):
    return lax.dot_general(a, b, (((0,), (0,)), ((), ())), preferred_element_type=F32)


def dot_nn(a, b):
    return lax.dot_general(a, b, (((1,), (0,)), ((), ())), preferred_element_type=F32)


def attend(q, k, v, do, mask):
    scores = mask(dot_nt(q, k))
    top = jnp.max(scores, axis=1, keepdims=True)
    e = jnp.exp2((scores - top) * EXP_SCALE)
    probs = e * (1.0 / jnp.sum(e, axis=1, keepdims=True))
    weights = probs.astype(BF16)
    attended = dot_nn(weights, v).astype(BF16)
    delta = jnp.sum(do.astype(F32) * attended.astype(F32), axis=1, keepdims=True)
    grads = (probs * (dot_nt(do, v) - delta)).astype(BF16)
    grad_q = (dot_nn(grads, k) * SCALE).astype(BF16)
    return attended, grad_q, weights, grads


def kernel(
    ranks,
    qs_hbm, ks_hbm, vs_hbm, ds_hbm, len_hbm, dest_hbm,
    ql_hbm, kl_hbm, vl_hbm, dl_hbm, order_hbm,
    os_ref, dqs_ref, dks_ref, dvs_ref, ol_ref, dql_ref, dkl_ref, dvl_ref,
    len_ref, dest_ref, order_ref, staged, short, arrived0, arrived1, placed, result, leaving, w_band, g_band, w_long, g_long, moved,
    int_sem, stage_sem, short_sem, own_sem, in_send, in_recv, out_send, out_recv, move_send, move_recv,
    cross_sem, go_sem, in0_sem, in2_sem, all_sem,
):
    dp = lax.axis_index("dp")
    me = lax.axis_index("ctx")
    partner = lax.rem(dp + ranks // 2, ranks)
    peers = {2: lax.rem(me + 2, 4), 3: 3 - me, 1: me + 1 - 2 * lax.rem(me, 2)}
    tokens = qs_hbm.shape[0]
    heads = qs_hbm.shape[1] // D
    mine, half = ql_hbm.shape[1], ql_hbm.shape[2]
    rows = mine * half
    arrived = (arrived0, arrived1)
    halves = arrived0.shape[1]
    total = halves * half
    longs = (ql_hbm, kl_hbm, vl_hbm, dl_hbm)
    long_outs = (ol_ref, dql_ref, dkl_ref, dvl_ref)

    int_copies = [
        pltpu.make_async_copy(src, dst, int_sem.at[i])
        for i, (src, dst) in enumerate(
            ((len_hbm, len_ref), (dest_hbm, dest_ref), (order_hbm, order_ref))
        )
    ]
    stage_copies = [
        pltpu.make_async_copy(longs[t], staged.at[t], stage_sem.at[t]) for t in range(4)
    ]
    short_copies = [
        pltpu.make_async_copy(src, short.at[t], short_sem.at[t])
        for t, src in enumerate((qs_hbm, ks_hbm, vs_hbm, ds_hbm))
    ]
    own_copies = []
    for h in range(heads):
        for t in range(4):
            cols = pl.ds(pl.multiple_of(me * heads * D + h * D, D), D)
            own_copies.append(
                pltpu.make_async_copy(
                    longs[t].at[0, :, :, cols],
                    arrived[h].at[t, pl.ds(me * mine, mine), :, :],
                    own_sem.at[h, t],
                )
            )

    def tell(sem, *cores, rank=dp):
        for core in cores:
            pl.semaphore_signal(sem, inc=1, device_id=(rank, core), device_id_type=MESH)

    barrier = pltpu.get_barrier_semaphore()

    @pl.when(me == 1)
    def _():
        tell(barrier, 0, 2, 3)

    @pl.when(me == 2)
    def _():
        tell(barrier, 3)
        tell(barrier, 2, rank=partner)

    @pl.when(me == 3)
    def _():
        tell(barrier, 1)

    for copy in stage_copies + int_copies + own_copies + short_copies:
        copy.start()
    for copy in stage_copies:
        copy.wait()
    pl.semaphore_wait(barrier, 1 + me // 2)

    @pl.when(me == 0)
    def _():
        tell(in0_sem, 1)
        pl.semaphore_wait(all_sem, 1)

    @pl.when(me == 3)
    def _():
        tell(in2_sem, 1)

    def inbound(h, t, r, peer):
        cols = pl.ds(pl.multiple_of(peer * heads * D + h * D, D), D)
        return pltpu.make_async_remote_copy(
            src_ref=staged.at[t, 0, :, :, cols],
            dst_ref=arrived[h].at[t, pl.ds(me * mine, mine), :, :],
            send_sem=in_send.at[h, t, r - 1],
            recv_sem=in_recv.at[h, t, r - 1],
            device_id=(dp, peer),
            device_id_type=MESH,
        )

    def send(h, r, peer):
        for t in range(4):
            inbound(h, t, r, peer).start()

    odd = lax.rem(me, 2)
    first, second = 3 - odd, 2 + odd
    first_peer = 3 - 2 * (me // 2)
    second_peer = first_peer - 1

    send(0, first, first_peer)

    @pl.when(me == 1)
    def _():
        pl.semaphore_wait(in2_sem, 1)

    @pl.when(me >= 2)
    def _():
        pl.semaphore_wait(all_sem, 1)

    send(0, second, second_peer)

    @pl.when(me == 1)
    def _():
        pl.semaphore_wait(in0_sem, 1)
        tell(all_sem, 0, 2, 3)

    @pl.when(me == LEADER)
    def _():
        tell(cross_sem, LEADER, rank=partner)

    send(0, 1, peers[1])
    for h in range(1, heads):
        send(h, first, first_peer)
        send(h, second, second_peer)
        send(h, 1, peers[1])
    in_copies = {
        (h, t, r): inbound(h, t, r, peer)
        for h in range(heads)
        for r, peer in peers.items()
        for t in range(4)
    }
    for copy in int_copies + short_copies:
        copy.wait()

    row = lax.broadcasted_iota(jnp.int32, (B, B), 0)
    col = lax.broadcasted_iota(jnp.int32, (B, B), 1)
    docs = len_ref.shape[0]
    lengths = [len_ref[j, dp] for j in range(docs)]
    tail = lengths[docs - 1]
    moves = dest_ref[docs - 1, dp] != dp
    tail_moved = jnp.where(moves, tail, 0)
    blocks = tokens // B

    def short_block(n):
        first = max(0, n - 2)
        start = jnp.zeros((B, B), jnp.int32)
        at = 0
        for j in range(docs - 1):
            at = at + lengths[j]
            start = jnp.where(row + n * B >= at, at, start)
        pieces = []
        for b in range(first, n + 1):
            piece = col + b * B >= start
            if b == n:
                piece = piece & (col <= row)
            pieces.append(piece)
        allowed = jnp.concatenate(pieces, axis=1) if len(pieces) > 1 else pieces[0]
        mask = lambda s: jnp.where(allowed, s, NEG)
        here = slice(n * B, (n + 1) * B)
        seen = slice(first * B, (n + 1) * B)
        outs = []
        for h in range(heads):
            c = slice(h * D, (h + 1) * D)
            attended, grad_q, weights, grads = attend(
                short[0, here, c], short[1, seen, c], short[2, seen, c], short[3, here, c], mask
            )
            dqs_ref[here, c] = grad_q
            for b in range(first, n + 1):
                to = slice((n - b) * B, (n - b + 1) * B)
                w_band[h, b, to, :] = weights[:, (b - first) * B : (b - first + 1) * B]
                g_band[h, b, to, :] = grads[:, (b - first) * B : (b - first + 1) * B]
            outs.append(attended)
        return here, jnp.concatenate(outs, axis=1)

    def short_keys(b):
        n = min(3, blocks - b) * B
        here = slice(b * B, (b + 1) * B)
        seen = slice(b * B, b * B + n)
        for h in range(heads):
            c = slice(h * D, (h + 1) * D)
            dks_ref[here, c] = (dot_tn(g_band[h, b, :n, :], short[0, seen, c]) * SCALE).astype(BF16)
            dvs_ref[here, c] = dot_tn(w_band[h, b, :n, :], short[3, seen, c]).astype(BF16)

    here, attended = short_block(blocks - 1)
    pick = (col == row + (B - tail_moved)) & (row < tail_moved)
    moved[...] = dot_nn(pick.astype(F32).astype(BF16), attended).astype(BF16)
    move = pltpu.make_async_remote_copy(
        src_ref=moved,
        dst_ref=os_ref.at[tokens : tokens + B, :],
        send_sem=move_send,
        recv_sem=move_recv,
        device_id=(partner, me),
        device_id_type=MESH,
    )
    keep = jnp.concatenate([row, row], axis=1) < B - tail_moved
    os_ref[here, :] = jnp.where(keep, attended.astype(F32), 0.0).astype(BF16)
    order = [order_ref[i] for i in range(halves)]
    found = []
    for p in range(halves):
        at = 0
        for i in range(halves):
            at = jnp.where(order[i] == p, i, at)
        found.append(at)
    lower = col <= row

    def outbound(h, t, r, peer):
        cols = pl.ds(pl.multiple_of(me * heads * D + h * D, D), D)
        return pltpu.make_async_remote_copy(
            src_ref=leaving.at[h, t, pl.ds(pl.multiple_of(peer * rows, rows), rows), :],
            dst_ref=long_outs[t].at[0, :, cols],
            send_sem=out_send.at[h, t, r - 1],
            recv_sem=out_recv.at[h, t, r - 1],
            device_id=(dp, peer),
            device_id_type=MESH,
        )

    def store(t, n, value):
        for i in range(B // half):
            result[t, n * (B // half) + i] = value[i * half : (i + 1) * half]

    def long_pass(h):
        for t in range(4):
            own_copies[h * 4 + t].wait()
        for r in peers:
            for t in range(4):
                in_copies[h, t, r].wait_recv()
        for t in range(4):
            for p in range(halves):
                placed[t, p * half : (p + 1) * half, :] = arrived[h][t, found[p]]
        for n in range(total // B):
            here = slice(n * B, (n + 1) * B)
            seen = slice(0, (n + 1) * B)

            def mask(s):
                last = jnp.where(lower, s[:, n * B :], NEG)
                return jnp.concatenate([s[:, : n * B], last], axis=1) if n else last

            attended, grad_q, weights, grads = attend(
                placed[0, here, :], placed[1, seen, :], placed[2, seen, :], placed[3, here, :], mask
            )
            store(0, n, attended)
            store(1, n, grad_q)
            w_long[here, seen] = weights
            g_long[here, seen] = grads
        for b in range(total // B):
            here = slice(b * B, (b + 1) * B)
            rest = slice(b * B, total)
            store(2, b, (dot_tn(g_long[rest, here], placed[0, rest, :]) * SCALE).astype(BF16))
            store(3, b, dot_tn(w_long[rest, here], placed[3, rest, :]).astype(BF16))
        for t in range(4):
            for i in range(halves):
                leaving[h, t, i * half : (i + 1) * half, :] = result[t, order[i]]
        cols = pl.ds(pl.multiple_of(me * heads * D + h * D, D), D)
        for r, peer in ((first, first_peer), (second, second_peer), (1, peers[1])):
            for t in range(4):
                outbound(h, t, r, peer).start()
        for t in range(4):
            long_outs[t][0, :, cols] = leaving[h, t, pl.ds(pl.multiple_of(me * rows, rows), rows), :]

    for n in range(blocks - 2, -1, -1):
        here, attended = short_block(n)
        os_ref[here, :] = attended
        short_keys(n + 1)
        if n == EARLY:
            long_pass(0)
        if n == blocks // 2:

            @pl.when(me == LEADER)
            def _():
                pl.semaphore_wait(cross_sem, 1)
                tell(go_sem, 0, 1, 3)

    short_keys(0)

    @pl.when(me != LEADER)
    def _():
        pl.semaphore_wait(go_sem, 1)

    move.start()
    for h in range(1, heads):
        long_pass(h)


    for copy in in_copies.values():
        copy.wait_send()
    move.wait()
    out_copies = {
        (h, t, r): outbound(h, t, r, peer)
        for h in range(heads)
        for r, peer in peers.items()
        for t in range(4)
    }
    for r in (1, 2, 3):
        for h in range(heads):
            for t in range(4):
                out_copies[h, t, r].wait_send()
    for r in (1, 2, 3):
        for h in range(heads):
            for t in range(4):
                out_copies[h, t, r].wait_recv()


def settle(*refs):
    count = (len(refs) - 1) // 2
    copies = [
        pltpu.make_async_copy(refs[i], refs[count + i], refs[-1].at[i]) for i in range(count)
    ]
    for copy in copies:
        copy.start()
    for copy in copies:
        copy.wait()


def shards(*args):
    q_short, q_long = args[0], args[6]
    halves = args[10].shape[0]
    tokens, width = q_short.shape
    heads = width // D
    _, rows, wide = q_long.shape
    ctx = lax.axis_size("ctx")
    total = rows * ctx
    blocks = tokens // B
    cut = [a.reshape(1, halves // ctx, total // halves, wide) for a in args[6:10]]
    args = args[:4] + (args[4].T, args[5].T, *cut, args[10])
    vmem = pl.BlockSpec(memory_space=pltpu.VMEM)
    hbm = pl.BlockSpec(memory_space=pl.ANY)
    dma = pltpu.SemaphoreType.DMA
    shapes = [(tokens + B, width)] + [(tokens, width)] * 3 + [(1, rows, wide)] * 4
    outs = pl.pallas_call(
        functools.partial(kernel, lax.axis_size("dp")),
        out_shape=tuple(pltpu.VMEM(s, BF16) for s in shapes),
        in_specs=[hbm] * 11,
        out_specs=(vmem,) * 8,
        scratch_shapes=[
            pltpu.SMEM(args[4].shape, jnp.int32),
            pltpu.SMEM(args[5].shape, jnp.int32),
            pltpu.SMEM(args[10].shape, jnp.int32),
            pltpu.VMEM((4,) + cut[0].shape, BF16),
            pltpu.VMEM((4, tokens, width), BF16),
            pltpu.VMEM((4, halves, total // halves, D), BF16),
            pltpu.VMEM((4, halves, total // halves, D), BF16),
            pltpu.VMEM((4, total, D), BF16),
            pltpu.VMEM((4, halves, total // halves, D), BF16),
            pltpu.VMEM((heads, 4, total, D), BF16),
            pltpu.VMEM((heads, blocks, 3 * B, B), BF16),
            pltpu.VMEM((heads, blocks, 3 * B, B), BF16),
            pltpu.VMEM((total, total), BF16),
            pltpu.VMEM((total, total), BF16),
            pltpu.VMEM((B, width), BF16),
            dma((3,)),
            dma((4,)),
            dma((4,)),
            dma((heads, 4)),
            dma((heads, 4, 3)),
            dma((heads, 4, 3)),
            dma((heads, 4, 3)),
            dma((heads, 4, 3)),
            dma,
            dma,
            pltpu.SemaphoreType.REGULAR,
            pltpu.SemaphoreType.REGULAR,
            pltpu.SemaphoreType.REGULAR,
            pltpu.SemaphoreType.REGULAR,
            pltpu.SemaphoreType.REGULAR,
        ],
        compiler_params=pltpu.CompilerParams(collective_id=0, has_side_effects=True),
        name="attention",
    )(*args)
    return pl.pallas_call(
        settle,
        out_shape=tuple(jax.ShapeDtypeStruct(s, BF16) for s in shapes),
        in_specs=[vmem] * 8,
        out_specs=(hbm,) * 8,
        scratch_shapes=[dma((8,))],
        name="settle",
    )(*[pltpu.with_memory_space_constraint(o, pltpu.VMEM) for o in outs])


def solution(mesh):
    short = P("dp", "ctx")
    long = P("dp", "ctx", None)
    return jax.shard_map(
        shards,
        mesh=mesh,
        in_specs=(short,) * 4 + (P(), P()) + (long,) * 4 + (P(),),
        out_specs=(short,) * 4 + (long,) * 4,
        check_vma=False,
    )
```

```python
import functools
import math

import jax
import jax.numpy as jnp
from jax import lax
from jax.experimental import pallas as pl
from jax.experimental.pallas import tpu as pltpu
from jax.sharding import PartitionSpec as P

D = 128
B = 128
NEG = -1e30
LEADER = 2
EARLY = 1
SCALE = D**-0.5
EXP_SCALE = SCALE * math.log2(math.e)
MESH = pl.DeviceIdType.MESH
BF16 = jnp.bfloat16
F32 = jnp.float32


def dot_nt(a, b):
    return lax.dot_general(a, b, (((1,), (1,)), ((), ())), preferred_element_type=F32)


def dot_tn(a, b):
    return lax.dot_general(a, b, (((0,), (0,)), ((), ())), preferred_element_type=F32)


def dot_nn(a, b):
    return lax.dot_general(a, b, (((1,), (0,)), ((), ())), preferred_element_type=F32)


def attend(q, k, v, do, mask):
    scores = mask(dot_nt(q, k))
    top = jnp.max(scores, axis=1, keepdims=True)
    e = jnp.exp2((scores - top) * EXP_SCALE)
    probs = e * (1.0 / jnp.sum(e, axis=1, keepdims=True))
    weights = probs.astype(BF16)
    attended = dot_nn(weights, v).astype(BF16)
    delta = jnp.sum(do.astype(F32) * attended.astype(F32), axis=1, keepdims=True)
    grads = (probs * (dot_nt(do, v) - delta)).astype(BF16)
    grad_q = (dot_nn(grads, k) * SCALE).astype(BF16)
    return attended, grad_q, weights, grads


def kernel(
    ranks,
    qs_hbm, ks_hbm, vs_hbm, ds_hbm, len_hbm, dest_hbm,
    ql_hbm, kl_hbm, vl_hbm, dl_hbm, order_hbm,
    os_ref, dqs_ref, dks_ref, dvs_ref, ol_ref, dql_ref, dkl_ref, dvl_ref,
    len_ref, dest_ref, order_ref, staged, short, arrived0, arrived1, placed, result, leaving, w_band, g_band, w_long, g_long, moved,
    int_sem, stage_sem, short_sem, own_sem, in_send, in_recv, out_send, out_recv, move_send, move_recv,
    cross_sem, go_sem, in0_sem, in2_sem, all_sem,
):
    dp = lax.axis_index("dp")
    me = lax.axis_index("ctx")
    partner = lax.rem(dp + ranks // 2, ranks)
    peers = {2: lax.rem(me + 2, 4), 3: 3 - me, 1: me + 1 - 2 * lax.rem(me, 2)}
    tokens = qs_hbm.shape[0]
    heads = qs_hbm.shape[1] // D
    mine, half = ql_hbm.shape[1], ql_hbm.shape[2]
    rows = mine * half
    arrived = (arrived0, arrived1)
    halves = arrived0.shape[1]
    total = halves * half
    longs = (ql_hbm, kl_hbm, vl_hbm, dl_hbm)
    long_outs = (ol_ref, dql_ref, dkl_ref, dvl_ref)

    int_copies = [
        pltpu.make_async_copy(src, dst, int_sem.at[i])
        for i, (src, dst) in enumerate(
            ((len_hbm, len_ref), (dest_hbm, dest_ref), (order_hbm, order_ref))
        )
    ]
    stage_copies = [
        pltpu.make_async_copy(longs[t], staged.at[t], stage_sem.at[t]) for t in range(4)
    ]
    short_copies = [
        pltpu.make_async_copy(src, short.at[t], short_sem.at[t])
        for t, src in enumerate((qs_hbm, ks_hbm, vs_hbm, ds_hbm))
    ]
    own_copies = []
    for h in range(heads):
        for t in range(4):
            cols = pl.ds(pl.multiple_of(me * heads * D + h * D, D), D)
            own_copies.append(
                pltpu.make_async_copy(
                    longs[t].at[0, :, :, cols],
                    arrived[h].at[t, pl.ds(me * mine, mine), :, :],
                    own_sem.at[h, t],
                )
            )

    def tell(sem, *cores, rank=dp):
        for core in cores:
            pl.semaphore_signal(sem, inc=1, device_id=(rank, core), device_id_type=MESH)

    barrier = pltpu.get_barrier_semaphore()

    @pl.when(me == 1)
    def _():
        tell(barrier, 0, 2, 3)

    @pl.when(me == 2)
    def _():
        tell(barrier, 3)
        tell(barrier, 2, rank=partner)

    @pl.when(me == 3)
    def _():
        tell(barrier, 1)

    for copy in stage_copies + int_copies + own_copies + short_copies:
        copy.start()
    for copy in stage_copies:
        copy.wait()
    pl.semaphore_wait(barrier, 1 + me // 2)

    @pl.when(me == 0)
    def _():
        tell(in0_sem, 1)
        pl.semaphore_wait(all_sem, 1)

    @pl.when(me == 3)
    def _():
        tell(in2_sem, 1)

    def inbound(h, t, r, peer):
        cols = pl.ds(pl.multiple_of(peer * heads * D + h * D, D), D)
        return pltpu.make_async_remote_copy(
            src_ref=staged.at[t, 0, :, :, cols],
            dst_ref=arrived[h].at[t, pl.ds(me * mine, mine), :, :],
            send_sem=in_send.at[h, t, r - 1],
            recv_sem=in_recv.at[h, t, r - 1],
            device_id=(dp, peer),
            device_id_type=MESH,
        )

    def send(h, r, peer):
        for t in range(4):
            inbound(h, t, r, peer).start()

    odd = lax.rem(me, 2)
    first, second = 3 - odd, 2 + odd
    first_peer = 3 - 2 * (me // 2)
    second_peer = first_peer - 1

    send(0, first, first_peer)

    @pl.when(me == 1)
    def _():
        pl.semaphore_wait(in2_sem, 1)

    @pl.when(me >= 2)
    def _():
        pl.semaphore_wait(all_sem, 1)

    send(0, second, second_peer)

    @pl.when(me == 1)
    def _():
        pl.semaphore_wait(in0_sem, 1)
        tell(all_sem, 0, 2, 3)

    @pl.when(me == LEADER)
    def _():
        tell(cross_sem, LEADER, rank=partner)

    for h in range(1, heads):
        send(h, first, first_peer)
        send(h, second, second_peer)
    for h in range(heads):
        send(h, 1, peers[1])
    in_copies = {
        (h, t, r): inbound(h, t, r, peer)
        for h in range(heads)
        for r, peer in peers.items()
        for t in range(4)
    }
    for copy in int_copies + short_copies:
        copy.wait()

    row = lax.broadcasted_iota(jnp.int32, (B, B), 0)
    col = lax.broadcasted_iota(jnp.int32, (B, B), 1)
    docs = len_ref.shape[0]
    lengths = [len_ref[j, dp] for j in range(docs)]
    tail = lengths[docs - 1]
    moves = dest_ref[docs - 1, dp] != dp
    tail_moved = jnp.where(moves, tail, 0)
    blocks = tokens // B

    def short_block(n):
        first = max(0, n - 2)
        start = jnp.zeros((B, B), jnp.int32)
        at = 0
        for j in range(docs - 1):
            at = at + lengths[j]
            start = jnp.where(row + n * B >= at, at, start)
        pieces = []
        for b in range(first, n + 1):
            piece = col + b * B >= start
            if b == n:
                piece = piece & (col <= row)
            pieces.append(piece)
        allowed = jnp.concatenate(pieces, axis=1) if len(pieces) > 1 else pieces[0]
        mask = lambda s: jnp.where(allowed, s, NEG)
        here = slice(n * B, (n + 1) * B)
        seen = slice(first * B, (n + 1) * B)
        outs = []
        for h in range(heads):
            c = slice(h * D, (h + 1) * D)
            attended, grad_q, weights, grads = attend(
                short[0, here, c], short[1, seen, c], short[2, seen, c], short[3, here, c], mask
            )
            dqs_ref[here, c] = grad_q
            for b in range(first, n + 1):
                to = slice((n - b) * B, (n - b + 1) * B)
                w_band[h, b, to, :] = weights[:, (b - first) * B : (b - first + 1) * B]
                g_band[h, b, to, :] = grads[:, (b - first) * B : (b - first + 1) * B]
            outs.append(attended)
        return here, jnp.concatenate(outs, axis=1)

    def short_keys(b):
        n = min(3, blocks - b) * B
        here = slice(b * B, (b + 1) * B)
        seen = slice(b * B, b * B + n)
        for h in range(heads):
            c = slice(h * D, (h + 1) * D)
            dks_ref[here, c] = (dot_tn(g_band[h, b, :n, :], short[0, seen, c]) * SCALE).astype(BF16)
            dvs_ref[here, c] = dot_tn(w_band[h, b, :n, :], short[3, seen, c]).astype(BF16)

    here, attended = short_block(blocks - 1)
    pick = (col == row + (B - tail_moved)) & (row < tail_moved)
    moved[...] = dot_nn(pick.astype(F32).astype(BF16), attended).astype(BF16)
    move = pltpu.make_async_remote_copy(
        src_ref=moved,
        dst_ref=os_ref.at[tokens : tokens + B, :],
        send_sem=move_send,
        recv_sem=move_recv,
        device_id=(partner, me),
        device_id_type=MESH,
    )
    keep = jnp.concatenate([row, row], axis=1) < B - tail_moved
    os_ref[here, :] = jnp.where(keep, attended.astype(F32), 0.0).astype(BF16)
    order = [order_ref[i] for i in range(halves)]
    found = []
    for p in range(halves):
        at = 0
        for i in range(halves):
            at = jnp.where(order[i] == p, i, at)
        found.append(at)
    lower = col <= row

    def outbound(h, t, r, peer):
        cols = pl.ds(pl.multiple_of(me * heads * D + h * D, D), D)
        return pltpu.make_async_remote_copy(
            src_ref=leaving.at[h, t, pl.ds(pl.multiple_of(peer * rows, rows), rows), :],
            dst_ref=long_outs[t].at[0, :, cols],
            send_sem=out_send.at[h, t, r - 1],
            recv_sem=out_recv.at[h, t, r - 1],
            device_id=(dp, peer),
            device_id_type=MESH,
        )

    def store(t, n, value):
        for i in range(B // half):
            result[t, n * (B // half) + i] = value[i * half : (i + 1) * half]

    def long_pass(h):
        for t in range(4):
            own_copies[h * 4 + t].wait()
        for r in peers:
            for t in range(4):
                in_copies[h, t, r].wait_recv()
        for t in range(4):
            for p in range(halves):
                placed[t, p * half : (p + 1) * half, :] = arrived[h][t, found[p]]
        for n in range(total // B):
            here = slice(n * B, (n + 1) * B)
            seen = slice(0, (n + 1) * B)

            def mask(s):
                last = jnp.where(lower, s[:, n * B :], NEG)
                return jnp.concatenate([s[:, : n * B], last], axis=1) if n else last

            attended, grad_q, weights, grads = attend(
                placed[0, here, :], placed[1, seen, :], placed[2, seen, :], placed[3, here, :], mask
            )
            store(0, n, attended)
            store(1, n, grad_q)
            w_long[here, seen] = weights
            g_long[here, seen] = grads
        for b in range(total // B):
            here = slice(b * B, (b + 1) * B)
            rest = slice(b * B, total)
            store(2, b, (dot_tn(g_long[rest, here], placed[0, rest, :]) * SCALE).astype(BF16))
            store(3, b, dot_tn(w_long[rest, here], placed[3, rest, :]).astype(BF16))
        for t in range(4):
            for i in range(halves):
                leaving[h, t, i * half : (i + 1) * half, :] = result[t, order[i]]
        cols = pl.ds(pl.multiple_of(me * heads * D + h * D, D), D)
        for r, peer in ((first, first_peer), (second, second_peer), (1, peers[1])):
            for t in range(4):
                outbound(h, t, r, peer).start()
        for t in range(4):
            long_outs[t][0, :, cols] = leaving[h, t, pl.ds(pl.multiple_of(me * rows, rows), rows), :]

    for n in range(blocks - 2, -1, -1):
        here, attended = short_block(n)
        os_ref[here, :] = attended
        short_keys(n + 1)
        if n == EARLY:
            long_pass(0)
        if n == blocks // 2:

            @pl.when(me == LEADER)
            def _():
                pl.semaphore_wait(cross_sem, 1)
                tell(go_sem, 0, 1, 3)

    short_keys(0)

    @pl.when(me != LEADER)
    def _():
        pl.semaphore_wait(go_sem, 1)

    move.start()
    for h in range(1, heads):
        long_pass(h)


    for copy in in_copies.values():
        copy.wait_send()
    move.wait()
    out_copies = {
        (h, t, r): outbound(h, t, r, peer)
        for h in range(heads)
        for r, peer in peers.items()
        for t in range(4)
    }
    for r in (1, 2, 3):
        for h in range(heads):
            for t in range(4):
                out_copies[h, t, r].wait_send()
    for r in (1, 2, 3):
        for h in range(heads):
            for t in range(4):
                out_copies[h, t, r].wait_recv()


def settle(*refs):
    count = (len(refs) - 1) // 2
    copies = [
        pltpu.make_async_copy(refs[i], refs[count + i], refs[-1].at[i]) for i in range(count)
    ]
    for copy in copies:
        copy.start()
    for copy in copies:
        copy.wait()


def shards(*args):
    q_short, q_long = args[0], args[6]
    halves = args[10].shape[0]
    tokens, width = q_short.shape
    heads = width // D
    _, rows, wide = q_long.shape
    ctx = lax.axis_size("ctx")
    total = rows * ctx
    blocks = tokens // B
    cut = [a.reshape(1, halves // ctx, total // halves, wide) for a in args[6:10]]
    args = args[:4] + (args[4].T, args[5].T, *cut, args[10])
    vmem = pl.BlockSpec(memory_space=pltpu.VMEM)
    hbm = pl.BlockSpec(memory_space=pl.ANY)
    dma = pltpu.SemaphoreType.DMA
    shapes = [(tokens + B, width)] + [(tokens, width)] * 3 + [(1, rows, wide)] * 4
    outs = pl.pallas_call(
        functools.partial(kernel, lax.axis_size("dp")),
        out_shape=tuple(pltpu.VMEM(s, BF16) for s in shapes),
        in_specs=[hbm] * 11,
        out_specs=(vmem,) * 8,
        scratch_shapes=[
            pltpu.SMEM(args[4].shape, jnp.int32),
            pltpu.SMEM(args[5].shape, jnp.int32),
            pltpu.SMEM(args[10].shape, jnp.int32),
            pltpu.VMEM((4,) + cut[0].shape, BF16),
            pltpu.VMEM((4, tokens, width), BF16),
            pltpu.VMEM((4, halves, total // halves, D), BF16),
            pltpu.VMEM((4, halves, total // halves, D), BF16),
            pltpu.VMEM((4, total, D), BF16),
            pltpu.VMEM((4, halves, total // halves, D), BF16),
            pltpu.VMEM((heads, 4, total, D), BF16),
            pltpu.VMEM((heads, blocks, 3 * B, B), BF16),
            pltpu.VMEM((heads, blocks, 3 * B, B), BF16),
            pltpu.VMEM((total, total), BF16),
            pltpu.VMEM((total, total), BF16),
            pltpu.VMEM((B, width), BF16),
            dma((3,)),
            dma((4,)),
            dma((4,)),
            dma((heads, 4)),
            dma((heads, 4, 3)),
            dma((heads, 4, 3)),
            dma((heads, 4, 3)),
            dma((heads, 4, 3)),
            dma,
            dma,
            pltpu.SemaphoreType.REGULAR,
            pltpu.SemaphoreType.REGULAR,
            pltpu.SemaphoreType.REGULAR,
            pltpu.SemaphoreType.REGULAR,
            pltpu.SemaphoreType.REGULAR,
        ],
        compiler_params=pltpu.CompilerParams(collective_id=0, has_side_effects=True),
        name="attention",
    )(*args)
    return pl.pallas_call(
        settle,
        out_shape=tuple(jax.ShapeDtypeStruct(s, BF16) for s in shapes),
        in_specs=[vmem] * 8,
        out_specs=(hbm,) * 8,
        scratch_shapes=[dma((8,))],
        name="settle",
    )(*[pltpu.with_memory_space_constraint(o, pltpu.VMEM) for o in outs])


def solution(mesh):
    short = P("dp", "ctx")
    long = P("dp", "ctx", None)
    return jax.shard_map(
        shards,
        mesh=mesh,
        in_specs=(short,) * 4 + (P(), P()) + (long,) * 4 + (P(),),
        out_specs=(short,) * 4 + (long,) * 4,
        check_vma=False,
    )
```
